128 devices in a mesh: rep: 2 (over core), dp: 64 (over x, y, z).
Axes of the slice: x: 4, y: 4, z: 4, core: 2. Of those that a mesh axis runs over, the one named last changes fastest.
Arguments:
- x: bfloat16 [128, 2048, 1024], P(('rep', 'dp')), parts along dimension 0
- dy: bfloat16 [128, 2048, 1024], P(('rep', 'dp')), parts along dimension 0
- wq: bfloat16 [1, 1024, 1536], P(None, 'dp')
- wk: bfloat16 [1, 1024, 256], P(None, 'dp')
- wv: bfloat16 [1, 1024, 256], P(None, 'dp')
- wo: bfloat16 [1, 1536, 1024], P(None, 'dp')
- w_gate: bfloat16 [1, 1024, 4096], P(None, 'dp')
- w_up: bfloat16 [1, 1024, 4096], P(None, 'dp')
- w_down: bfloat16 [1, 4096, 1024], P(None, 'dp')
Outputs:
- output 1: bfloat16 [128, 2048, 1024], P(('rep', 'dp')), parts along dimension 0
- output 2: bfloat16 [2, 1024, 1536], P('rep', 'dp'), parts along dimension 0
- output 3: bfloat16 [2, 1024, 256], P('rep', 'dp'), parts along dimension 0
- output 4: bfloat16 [2, 1024, 256], P('rep', 'dp'), parts along dimension 0
- output 5: bfloat16 [2, 1536, 1024], P('rep', 'dp'), parts along dimension 0
- output 6: bfloat16 [2, 1024, 4096], P('rep', 'dp'), parts along dimension 0
- output 7: bfloat16 [2, 1024, 4096], P('rep', 'dp'), parts along dimension 0
- output 8: bfloat16 [2, 4096, 1024], P('rep', 'dp'), parts along dimension 0
There are 2 independent parts. The reference program is written for one: setup_inputs(seed, part) draws one part's arguments, and reference() takes and returns one part's arrays. A program takes and returns all parts, laid end to end along the dimension named above; an argument that names none is the same for every part.
All inputs are finite; a program needn't handle non-finite values.
Results may differ from the reference program's by a relative error of at most 0.024.
Values are sent between devices in bfloat16 or wider.
A program may use at most 1.5 GiB of HBM per device.

```python
import jax
import jax.numpy as jnp
from jax import lax

SEQUENCES = 64
TOKENS = 2048
D = 1024
HEADS = 12
KV_HEADS = 2
HEAD = 128
FF = 4096
LAYERS = 1
THETA = 10000
NAMES = ("wq", "wk", "wv", "wo", "w_gate", "w_up", "w_down")
SHAPES = {
    "wq": (LAYERS, D, HEADS * HEAD),
    "wk": (LAYERS, D, KV_HEADS * HEAD),
    "wv": (LAYERS, D, KV_HEADS * HEAD),
    "wo": (LAYERS, HEADS * HEAD, D),
    "w_gate": (LAYERS, D, FF),
    "w_up": (LAYERS, D, FF),
    "w_down": (LAYERS, FF, D),
}


def bump(key, n, height):
    away = (jnp.arange(n, dtype=jnp.int32) - jax.random.randint(key, (), 0, n, jnp.int32)) % n
    return jnp.where(away < n // 8, height, 1.0)


def together(key, own, strength):
    shared = jax.random.normal(key, own.shape[1:], jnp.float32)
    return (own + strength * shared) * lax.rsqrt(1 + strength * strength)


def setup_inputs(seed: int = 0, part: int = 0) -> dict:
    kx, kdy, ka, kb, kz, kf, kh, kl, *keys = jax.random.split(jax.random.key(seed), 8 + 3 * len(NAMES))
    kx, kdy, ka, kb = (jax.random.fold_in(k, part) for k in (kx, kdy, ka, kb))
    kw, km, kv = (keys[i::3] for i in range(3))
    shape = (SEQUENCES, TOKENS, D)
    much_x, much_dy = jax.random.uniform(kz, (2,), jnp.float32, 0.0, 1.0)
    loud = 2.0 ** jax.random.uniform(jax.random.fold_in(kz, 1), (), jnp.float32, -1.0, 2.0)
    layers = 2.0 ** jax.random.uniform(kl, (LAYERS, 1, 1), jnp.float32, -1.0, 1.0)
    times = {"wq": 1.0, "wk": 1.0, "wv": 2.0, "wo": layers, "w_gate": 1.0, "w_up": bump(kh, FF, 4.0), "w_down": layers}
    x = together(ka, jax.random.normal(kx, shape, jnp.float32), much_x) * bump(kf, D, 4.0)
    dy = together(kb, jax.random.normal(kdy, shape, jnp.float32), much_dy)
    drawn = {"x": x.astype(jnp.bfloat16), "dy": (loud * dy * (SEQUENCES * TOKENS) ** -0.5).astype(jnp.bfloat16)}
    for key, name in zip(kw, NAMES, strict=True):
        drawn[name] = (jax.random.normal(key, SHAPES[name], jnp.float32) * SHAPES[name][1] ** -0.5 * times[name]).astype(jnp.bfloat16)
    return drawn


def matmul(a, w):
    return jnp.dot(a, w, preferred_element_type=jnp.float32).astype(jnp.bfloat16)


def normed(h):
    wide = h.astype(jnp.float32)
    scale = lax.rsqrt(jnp.mean(wide**2, -1, keepdims=True) + 1e-6)
    return (wide * scale).astype(jnp.bfloat16)


def turned(t, theta):
    half = t.shape[-1] // 2
    angle = jnp.arange(t.shape[0], dtype=jnp.float32)[:, None] * theta ** (-jnp.arange(half, dtype=jnp.float32) / half)
    cos, sin = jnp.cos(angle)[:, None], jnp.sin(angle)[:, None]
    a, b = t[..., :half].astype(jnp.float32), t[..., half:].astype(jnp.float32)
    return jnp.concatenate([a * cos - b * sin, b * cos + a * sin], -1).astype(jnp.bfloat16)


def seen_by(q, k, v):
    tokens, kv = q.shape[0], k.shape[1]
    q = q.reshape(tokens, kv, -1, q.shape[-1])
    scores = jnp.einsum("tgsd,ugd->gstu", q.astype(jnp.float32), k.astype(jnp.float32)) * q.shape[-1] ** -0.5
    place = jnp.arange(tokens)
    weights = jax.nn.softmax(jnp.where(place[:, None] >= place, scores, -jnp.inf), -1).astype(jnp.bfloat16)
    return jnp.einsum("gstu,ugd->tgsd", weights.astype(jnp.float32), v.astype(jnp.float32)).astype(jnp.bfloat16).reshape(tokens, -1)


def layer(h, w):
    a = normed(h)
    q, k = (turned(matmul(a, w[name]).reshape(h.shape[0], -1, HEAD), THETA) for name in ("wq", "wk"))
    h = h + matmul(seen_by(q, k, matmul(a, w["wv"]).reshape(h.shape[0], -1, HEAD)), w["wo"])
    b = normed(h)
    gate = jnp.dot(b, w["w_gate"], preferred_element_type=jnp.float32)
    up = jnp.dot(b, w["w_up"], preferred_element_type=jnp.float32)
    return h + matmul((jax.nn.silu(gate) * up).astype(jnp.bfloat16), w["w_down"])


def stack(weights, h):
    return lax.scan(lambda h, w: (layer(h, w), None), h, weights)[0]


def reference(x, dy, wq, wk, wv, wo, w_gate, w_up, w_down):
    weights = dict(zip(NAMES, (wq, wk, wv, wo, w_gate, w_up, w_down), strict=True))

    def take(so_far, sequence):
        h, by_y = sequence
        _, back = jax.vjp(stack, weights, h)
        by_weights, by_h = back(by_y)
        return jax.tree.map(lambda total, term: total + term.astype(jnp.float32), so_far, by_weights), by_h

    none_yet = {name: jnp.zeros(w.shape, jnp.float32) for name, w in weights.items()}
    by_weights, by_x = lax.scan(take, none_yet, (x, dy))
    return (by_x, *(by_weights[name].astype(jnp.bfloat16) for name in NAMES))
```

```python
import functools
import math

import jax
import jax.numpy as jnp
from jax import lax
from jax.experimental import pallas as pl
from jax.experimental.pallas import tpu as pltpu
from jax.sharding import PartitionSpec as P

MESH = pl.DeviceIdType.MESH
BF16, F32 = jnp.bfloat16, jnp.float32
HEAD = 128
HEADS = 12
KV = 2
GROUP = HEADS // KV
THETA = 10000
EPS = 1e-6
LOG2E = 1.4426950408889634
HIDDEN = -2e30
SIDE = 4
ORDERS = ((0, 1, 2), (1, 2, 0), (2, 0, 1))


def _dot(a, b, ca, cb):
    return lax.dot_general(a, b, (((ca,), (cb,)), ((), ())), preferred_element_type=F32)


class Place:
    def __init__(self):
        self.rep, p = lax.axis_index("rep"), lax.axis_index("dp")
        self.at = (p // 16, (p // 4) % 4, p % 4)

    def step(self, dim, by):
        return (self.at[dim] + by) % SIDE

    def device(self, dim, by):
        x, y, z = (self.step(d, by) if d == dim else self.at[d] for d in range(3))
        return (self.rep, x * 16 + y * 4 + z)

    def partner(self):
        x, y, z = self.at
        return (1 - self.rep, x * 16 + y * 4 + z)


def meet(place, far, partner):
    others = [place.device(d, by) for d in range(3) for by in ((1, 3, 2) if far else (1, 3))]
    if partner:
        others.append(place.partner())
    barrier = pltpu.get_barrier_semaphore()
    for other in others:
        pl.semaphore_signal(barrier, inc=1, device_id=other, device_id_type=MESH)
    pl.semaphore_wait(barrier, len(others))


COPIES = 15
GATHER_STAGES = 7


class Gather:
    def __init__(self, place, shard, full, colour, first, width, send, recv, local):
        self.place, self.shard, self.full, self.dims = place, shard, full, ORDERS[colour]
        half = shard.shape[-1] // 2
        self.cols = pl.ds(pl.multiple_of(place.rep * half + first, 128), width)
        self.send, self.recv, self.local = send, recv, local

    def blocks(self, **where):
        index = [slice(None)] * 3
        for name, value in where.items():
            index[self.dims[int(name[1])]] = value
        return self.full.at[(*index, slice(None), self.cols)]

    def copies(self):
        p, (a, b, c) = self.place, self.dims
        ia, ib, ic = (p.at[d] for d in self.dims)
        low, high = pl.ds(0, 2), pl.ds(2, 2)
        own = self.blocks(d0=ia, d1=ib, d2=ic)
        mine = self.shard.at[:, self.cols]
        out = [(mine, own, p.device(a, by)) for by in (1, 3, 2)]
        row = self.blocks(d1=ib, d2=ic)
        out += [(row, row, p.device(b, by)) for by in (1, 3)]
        for by, part in ((1, low), (3, high)):
            got = self.blocks(d0=part, d1=p.step(b, -by), d2=ic)
            out.append((got, got, p.device(b, by)))
        plane = self.blocks(d2=ic)
        out += [(plane, plane, p.device(c, by)) for by in (1, 3)]
        for by, part in ((1, low), (3, high)):
            got = self.blocks(d0=part, d2=p.step(c, -by))
            out.append((got, got, p.device(c, by)))
        for by in (0, 1, 3, 2):
            got = self.blocks(d2=p.step(c, by))
            out.append((got, got, p.partner()))
        return out

    def copy(self, n):
        src, dst, device = self.copies()[n]
        return pltpu.make_async_remote_copy(src_ref=src, dst_ref=dst, send_sem=self.send.at[n], recv_sem=self.recv.at[n], device_id=device,
                                            device_id_type=MESH)

    def keep(self):
        ia, ib, ic = (self.place.at[d] for d in self.dims)
        return pltpu.make_async_copy(self.shard.at[:, self.cols], self.blocks(d0=ia, d1=ib, d2=ic), self.local)

    def start(self, *which):
        for n in which:
            self.copy(n).start()

    def got(self, *which):
        for n in which:
            self.copy(n).wait_recv()

    def stage(self, s):
        if s == 0:
            self.keep().start()
            self.start(0, 1, 2)
        elif s == 1:
            self.keep().wait()
            self.got(0, 1, 2)
            self.start(3, 4)
        elif s == 2:
            self.got(3, 4)
            self.start(5, 6)
        elif s == 3:
            self.got(5, 6)
            self.start(7, 8, 11)
        elif s == 4:
            self.got(7, 8)
            self.start(9, 10, 12, 13)
        elif s == 5:
            self.got(9, 10)
            self.start(14)
        else:
            self.got(11, 12, 13, 14)
            for n in range(COPIES):
                self.copy(n).wait_send()


SCATTER_STAGES = 7
SLOTS = 3


class Scatter:
    def __init__(self, place, grad, out, colour, first, width, rounds, scratch):
        self.place, self.grad, self.out, self.first, self.width, self.rounds = place, grad, out, first, width, rounds
        self.dims = ORDERS[colour]
        self.left = [[d for d in range(3) if d not in self.dims[: n + 1]] for n in range(3)]
        (self.own, self.rel, self.ra0, self.rb0, self.x1, self.ra1, self.rb1, self.x2, self.ra2, self.rb2, self.total, self.send0, self.recv0,
         self.send1, self.recv1, self.load, self.save) = scratch

    @staticmethod
    def scratch(rows, width, rounds):
        slots = min(SLOTS, rounds)
        b0, b1, b2 = (4, 4, rows, width), (4, rows, width), (rows, width)
        h0, h1, h2 = (2, 4, rows, width), (2, rows, width), (rows // 2, width) if width % 256 else (rows, width // 2)
        vmem = lambda *shape: pltpu.VMEM(shape, BF16)
        dma = pltpu.SemaphoreType.DMA
        return [vmem(slots, *b0), vmem(slots, 2, *h0), vmem(slots, 2, *h0), vmem(slots, 2, *b0), vmem(rounds, *b0), vmem(rounds, 2, *h1),
                vmem(rounds, 2, *b1), vmem(rounds, *b1), vmem(rounds, 2, *h2), vmem(rounds, 2, *b2), vmem(rounds, *b2), dma((slots, 6)),
                dma((slots, 6)), dma((rounds, 2, 6)), dma((rounds, 2, 6)), dma((slots, 3)), dma((rounds,))]

    def slot(self, r):
        return r % min(SLOTS, self.rounds)

    def part(self, n, half):
        if n < 2:
            return (pl.ds(2 * half, 2),)
        if self.width % 256:
            rows = self.out.shape[0] // 2
            return (pl.ds(half * rows, rows), slice(None))
        return (slice(None), pl.ds(half * (self.width // 2), self.width // 2))

    def x(self, n, r, j, half=None):
        d = self.dims[n]
        rest = () if half is None else self.part(n, half)
        if n == 0:
            cols = pl.ds(pl.multiple_of(self.first + r * self.width, 128), self.width)
            index = [slice(None)] * 3
            index[d] = j
            if half is not None:
                index[self.left[0][0]] = rest[0]
            return self.grad.at[(*index, slice(None), cols)]
        if n == 1:
            index = [slice(None)] * 2
            index[self.left[0].index(d)] = j
            if half is not None:
                index[self.left[0].index(self.left[1][0])] = rest[0]
            return self.x1.at[(r, *index)]
        return self.x2.at[(r, j, *rest)]

    def copy(self, n, r, k):
        p, d = self.place, self.dims[n]
        by, half = (1, 3)[k % 2], (0, 1, 1, 0, 0, 1)[k]
        s = self.slot(r)
        ra, rb = ((self.ra0.at[s], self.rb0.at[s]), (self.ra1.at[r], self.rb1.at[r]), (self.ra2.at[r], self.rb2.at[r]))[n]
        send, recv = (self.send0.at[s], self.recv0.at[s]) if n == 0 else (self.send1.at[r, n - 1], self.recv1.at[r, n - 1])
        if k < 2:
            src, dst = self.x(n, r, p.step(d, 2), half), ra.at[k]
        else:
            dst = rb.at[(k % 2, *self.part(n, half))]
            src = self.rel.at[s, k - 4] if n == 0 and k >= 4 else self.x(n, r, p.step(d, by), half)
        return pltpu.make_async_remote_copy(src_ref=src, dst_ref=dst, send_sem=send.at[k], recv_sem=recv.at[k], device_id=p.device(d, by),
                                            device_id_type=MESH)

    def loading(self, r, k):
        p, d, s = self.place, self.dims[0], self.slot(r)
        src = self.x(0, r, p.at[d]) if k == 2 else self.x(0, r, p.step(d, (1, 3)[k]), k)
        return pltpu.make_async_copy(src, self.own.at[s] if k == 2 else self.rel.at[s, k], self.load.at[s, k])

    def saving(self, r):
        cols = pl.ds(pl.multiple_of(self.first + r * self.width, 128), self.width)
        return pltpu.make_async_copy(self.total.at[r], self.out.at[:, cols], self.save.at[r])

    def relay(self, n, r):
        p, d, s = self.place, self.dims[n], self.slot(r)
        for h in range(2):
            ra = (self.ra0.at[s, h], self.ra1.at[r, h], self.ra2.at[r, h])[n]
            mine = self.rel.at[s, h] if n == 0 else self.x(n, r, p.step(d, (1, 3)[h]), h)
            _add(mine, [mine, ra])

    def finish(self, n, r):
        p, d, s = self.place, self.dims[n], self.slot(r)
        rb = (self.rb0.at[s], self.rb1.at[r], self.rb2.at[r])[n]
        mine = self.own.at[s] if n == 0 else self.x(n, r, p.at[d])
        _add((self.x1.at[r], self.x2.at[r], self.total.at[r])[n], [mine, rb.at[0], rb.at[1]])

    def begin(self, n, r):
        for k in range(4):
            self.copy(n, r, k).start()

    def stage(self, s, r):
        if s == 0:
            for k in range(3):
                self.loading(r, k).start()
            self.begin(0, r)
            return
        n = (s - 1) // 2
        if s % 2:
            for k in (0, 1):
                self.copy(n, r, k).wait_recv()
            if n == 0:
                self.loading(r, 0).wait()
                self.loading(r, 1).wait()
            self.relay(n, r)
            for k in (4, 5):
                self.copy(n, r, k).start()
            return
        for k in (2, 3, 4, 5):
            self.copy(n, r, k).wait_recv()
        if n == 0:
            self.loading(r, 2).wait()
        self.finish(n, r)
        if n < 2:
            self.begin(n + 1, r)
        else:
            self.saving(r).start()
        for k in range(6):
            self.copy(n, r, k).wait_send()

    def end(self):
        for r in range(self.rounds):
            self.saving(r).wait()


def _add(out, terms):
    lead = out.shape[:-2]
    if not lead:
        out[...] = sum(t[...].astype(F32) for t in terms).astype(out.dtype)
        return

    def one(i, _):
        index = []
        for size in reversed(lead):
            index.insert(0, i % size)
            i = i // size
        index = tuple(index)
        out[index] = sum(t[index].astype(F32) for t in terms).astype(out.dtype)

    lax.fori_loop(0, math.prod(lead), one, None)


def _first(x_ref, q_in, k_in, v_in, a_ref, q_out, k_out, v_out, send, recv, local):
    place = Place()
    job = lambda n, shard, full, colour, first, width: Gather(place, shard, full, colour, first, width, send.at[n], recv.at[n], local.at[n])
    wide = q_in.shape[1] // 4
    jobs = [job(0, q_in, q_out, 0, 0, wide), job(1, q_in, q_out, 1, wide, wide), job(2, k_in, k_out, 2, 0, k_in.shape[1] // 2),
            job(3, v_in, v_out, 2, 0, v_in.shape[1] // 2)]
    meet(place, True, True)
    for j in jobs:
        j.stage(0)

    rows = 128

    def norm(i, _):
        here = pl.ds(pl.multiple_of(i * rows, rows), rows)
        wide = x_ref[here, :].astype(F32)
        a_ref[here, :] = (wide * lax.rsqrt(jnp.mean(wide * wide, -1, keepdims=True) + EPS)).astype(BF16)

    lax.fori_loop(0, x_ref.shape[0] // rows, norm, None)
    for s in range(1, GATHER_STAGES):
        for j in jobs:
            j.stage(s)


def torus(w):
    return (SIDE, SIDE, SIDE, w.shape[0], w.shape[1])


def first(x, wq, wk, wv):
    anywhere = pl.BlockSpec(memory_space=pl.ANY)
    vmem = pl.BlockSpec(memory_space=pltpu.VMEM)
    dma = pltpu.SemaphoreType.DMA
    full = lambda w: jax.ShapeDtypeStruct(torus(w), BF16)
    out = pl.pallas_call(
        _first,
        out_shape=[jax.ShapeDtypeStruct(x.shape, BF16), full(wq), full(wk), full(wv)],
        in_specs=[vmem, anywhere, anywhere, anywhere],
        out_specs=[vmem, anywhere, anywhere, anywhere],
        scratch_shapes=[dma((4, COPIES)), dma((4, COPIES)), dma((4,))],
        compiler_params=pltpu.CompilerParams(collective_id=0, has_side_effects=True, vmem_limit_bytes=32 * 2**20),
        name="first",
    )(x, wq, wk, wv)
    return out[0], [w.reshape(-1, w.shape[-1]) for w in out[1:]]


def _steps(i, per):
    m, k = i // per, i % per
    return per * (m * (m + 1) // 2) + k * (m + 1)


def _turn(x, cos, sin):
    return x * cos + pltpu.roll(x, HEAD // 2, 1) * sin


def _head(h):
    return slice(h * HEAD, (h + 1) * HEAD)


FWD_Q, FWD_K, FWD_STRIP = 256, 512, 2
BWD_Q, BWD_K, BWD_STRIP = 128, 512, 3
FWD_WHEN = (0, 2, 4, 7, 10, 14, 18)


def _attend(q_ref, k_ref, v_ref, cos_ref, sin_ref, o_in, g_in, u_in, d_in, out_ref, lse_ref, qr_ref, kr_ref, o_out, g_out, u_out, d_out,
            q_s, top_s, mix_s, gap_s, send, recv, local):
    i = pl.program_id(0)
    bq, bk, per = q_ref.shape[0], FWD_K, FWD_K // FWD_Q
    wide = FWD_STRIP * bq
    e = HEAD**-0.5 * LOG2E
    strips = HEADS // FWD_STRIP
    place = Place()
    job = lambda n, shard, full, colour, first, width: Gather(place, shard, full, colour, first, width, send.at[n], recv.at[n], local.at[n])
    jobs = [job(0, o_in, o_out, 0, 0, 128), job(1, o_in, o_out, 1, 128, 128), job(2, o_in, o_out, 2, 256, 256),
            job(3, g_in, g_out, 0, 0, g_in.shape[1] // 2), job(4, u_in, u_out, 1, 0, u_in.shape[1] // 2),
            job(5, d_in, d_out, 2, 0, d_in.shape[1] // 2)]

    @pl.when(i == 0)
    def _():
        meet(place, True, True)

    def hook(t):
        for s, due in enumerate(FWD_WHEN):

            @pl.when(t == due)
            def _(s=s):
                for j in jobs:
                    j.stage(s)

    @pl.when(i == 0)
    def _():
        gap_s[...] = lax.broadcasted_iota(jnp.int32, gap_s.shape, 1) % bq - lax.broadcasted_iota(jnp.int32, gap_s.shape, 0)

        def turn(n, _):
            here = pl.ds(pl.multiple_of(n * 256, 256), 256)
            for h in range(KV):
                kr_ref[here, _head(h)] = _turn(k_ref[here, _head(h)].astype(F32), cos_ref[here, :], sin_ref[here, :]).astype(BF16)

        lax.fori_loop(0, k_ref.shape[0] // 256, turn, None)

    rows = pl.ds(pl.multiple_of(i * bq, bq), bq)
    cos, sin = cos_ref[rows, :], sin_ref[rows, :]
    for h in range(HEADS):
        turned = _turn(q_ref[:, _head(h)].astype(F32), cos, sin).astype(BF16)
        qr_ref[:, _head(h)] = turned
        q_s[h // FWD_STRIP, (h % FWD_STRIP) * bq : (h % FWD_STRIP + 1) * bq, :] = turned
    top_s[...] = jnp.full(top_s.shape, HIDDEN / 2, F32)
    mix_s[...] = jnp.zeros(mix_s.shape, F32)
    ones = jnp.ones((8, bk), BF16)

    def block(j, masked):
        here = pl.ds(pl.multiple_of(j * bk, bk), bk)
        kv = lambda n: _head(n * FWD_STRIP // GROUP)
        scores = [_dot(kr_ref[here, kv(n)], q_s[n], 1, 1) for n in range(strips)]
        ok = gap_s[...] >= j * bk - i * bq if masked else None
        weights, keeps = [], []
        for n, s in enumerate(scores):
            if masked:
                s = jnp.where(ok, s, HIDDEN)
            old = top_s[n : n + 1, :]
            top = jnp.maximum(old, s.max(axis=0, keepdims=True))
            top_s[n : n + 1, :] = top
            weights.append(jnp.exp2((s - top) * e).astype(BF16))
            keeps.append(jnp.exp2((old - top) * e))
        for n, (p, keep) in enumerate(zip(weights, keeps)):
            values = jnp.concatenate([v_ref[here, kv(n)].T, ones], axis=0)
            mix_s[n] = mix_s[n] * keep + _dot(values, p, 1, 0)

    whole, base = i // per, _steps(i, per)
    blocks = q_tokens(cos_ref) // bq

    def step(j, _):
        @pl.when(j <= whole)
        def _():
            hook(base + j)

        @pl.when(j < whole)
        def _():
            block(j, False)

        @pl.when(j == whole)
        def _():
            block(j, True)

    lax.fori_loop(0, blocks // per, step, None)
    done = _steps(blocks, per)
    if FWD_WHEN[-1] >= done:

        @pl.when(i == blocks - 1)
        def _():
            lax.fori_loop(done, FWD_WHEN[-1] + 1, lambda t, _: hook(t), None)

    for h in range(HEADS):
        n, at = h // FWD_STRIP, slice((h % FWD_STRIP) * bq, (h % FWD_STRIP + 1) * bq)
        total = mix_s[n, HEAD : HEAD + 1, at]
        out_ref[:, _head(h)] = (mix_s[n, :HEAD, at] * (1 / total)).T.astype(BF16)
        lse_ref[h : h + 1, :] = (top_s[n : n + 1, at] * HEAD**-0.5 + jnp.log(total)) * LOG2E


def q_tokens(ref):
    return ref.shape[0]


def attend(q, k, v, cos, sin, wo, wg, wu, wd):
    tokens = q.shape[0]
    anywhere = pl.BlockSpec(memory_space=pl.ANY)
    dma = pltpu.SemaphoreType.DMA
    block = pl.BlockSpec((FWD_Q, HEADS * HEAD), lambda i: (i, 0))
    fixed = lambda a: pl.BlockSpec(a.shape, lambda i: (0, 0))
    full = lambda w: jax.ShapeDtypeStruct(torus(w), BF16)
    wide = FWD_STRIP * FWD_Q
    out = pl.pallas_call(
        _attend,
        grid=(tokens // FWD_Q,),
        out_shape=[jax.ShapeDtypeStruct(q.shape, BF16), jax.ShapeDtypeStruct((HEADS, tokens), F32), jax.ShapeDtypeStruct(q.shape, BF16),
                   jax.ShapeDtypeStruct(k.shape, BF16), full(wo), full(wg), full(wu), full(wd)],
        in_specs=[block, fixed(k), fixed(v), fixed(cos), fixed(sin)] + [anywhere] * 4,
        out_specs=[block, pl.BlockSpec((HEADS, FWD_Q), lambda i: (0, i)), block, fixed(k)] + [anywhere] * 4,
        scratch_shapes=[pltpu.VMEM((HEADS // FWD_STRIP, wide, HEAD), BF16), pltpu.VMEM((HEADS // FWD_STRIP, wide), F32),
                        pltpu.VMEM((HEADS // FWD_STRIP, HEAD + 8, wide), F32), pltpu.VMEM((FWD_K, wide), jnp.int32),
                        dma((6, COPIES)), dma((6, COPIES)), dma((6,))],
        compiler_params=pltpu.CompilerParams(collective_id=1, has_side_effects=True, vmem_limit_bytes=56 * 2**20,
                                             dimension_semantics=("arbitrary",)),
        name="attend",
    )(q, k, v, cos, sin, wo, wg, wu, wd)
    return out[:4], [w.reshape(-1, w.shape[-1]) for w in out[4:]]


BWD_ROUNDS = 8
BWD_EVERY = 4
BWD_WHEN = (0, 3, 5, 8, 11, 13, 15)


def _attend_bwd(q_ref, k_ref, v_ref, o_ref, do_ref, lse_ref, cos_ref, sin_ref, gg, gu, gd, dq_ref, dk_ref, dv_ref, og, ou, od,
                dq_s, dk_s, dv_s, gap_s, *scratch):
    i = pl.program_id(0)
    bq, bk, per = q_ref.shape[0], BWD_K, BWD_K // BWD_Q
    strips = HEADS // BWD_STRIP
    wide = BWD_STRIP * bq
    scale = HEAD**-0.5
    e = scale * LOG2E
    place = Place()
    each = len(scratch) // 3
    jobs = [Scatter(place, g, o, colour, 0, g.shape[-1] // BWD_ROUNDS, BWD_ROUNDS, scratch[colour * each : (colour + 1) * each])
            for colour, (g, o) in enumerate(((gg, og), (gu, ou), (gd, od)))]

    @pl.when(i == 0)
    def _():
        meet(place, False, False)
        gap_s[...] = lax.broadcasted_iota(jnp.int32, gap_s.shape, 1) % bq - lax.broadcasted_iota(jnp.int32, gap_s.shape, 0)
        dk_s[...] = jnp.zeros(dk_s.shape, F32)
        dv_s[...] = jnp.zeros(dv_s.shape, F32)

    def hook(t):
        for s in reversed(range(SCATTER_STAGES)):
            since = t - BWD_WHEN[s]

            @pl.when((since >= 0) & (since < BWD_EVERY * BWD_ROUNDS) & (since % BWD_EVERY == 0))
            def _(s=s, since=since):
                for j in jobs:
                    j.stage(s, since // BWD_EVERY)

    dq_s[...] = jnp.zeros(dq_s.shape, F32)
    heads = lambda n: range(n * BWD_STRIP, (n + 1) * BWD_STRIP)
    deltas, lses = [], []
    for n in range(strips):
        products = [do_ref[:, _head(h)].astype(F32) * o_ref[:, _head(h)].astype(F32) for h in heads(n)]
        deltas.append(jnp.concatenate([x.T.sum(axis=0, keepdims=True) for x in products], axis=1))
        lses.append(jnp.concatenate([lse_ref[h : h + 1, :] for h in heads(n)], axis=1))

    def block(j, masked):
        here = pl.ds(pl.multiple_of(j * bk, bk), bk)
        kv = [n * BWD_STRIP // GROUP for n in range(strips)]
        qs = [jnp.concatenate([q_ref[:, _head(h)] for h in heads(n)], axis=0) for n in range(strips)]
        dos = [jnp.concatenate([do_ref[:, _head(h)] for h in heads(n)], axis=0) for n in range(strips)]
        scores = [_dot(k_ref[here, _head(kv[n])], qs[n], 1, 1) for n in range(strips)]
        dps = [_dot(v_ref[here, _head(kv[n])], dos[n], 1, 1) for n in range(strips)]
        ok = gap_s[...] >= j * bk - i * bq if masked else None
        for n in range(strips):
            p = jnp.exp2(scores[n] * e - lses[n])
            if masked:
                p = jnp.where(ok, p, 0.0)
            ds = (p * (dps[n] - deltas[n])).astype(BF16)
            dv_s[kv[n], here, :] += _dot(p.astype(BF16), dos[n], 1, 0)
            dk_s[kv[n], here, :] += _dot(ds, qs[n], 1, 0)
            dq_s[n] += _dot(k_ref[here, _head(kv[n])].T, ds, 1, 0)

    whole, base = i // per, _steps(i, per)
    blocks = q_tokens(cos_ref) // bq

    def step(j, _):
        @pl.when(j <= whole)
        def _():
            hook(base + j)

        @pl.when(j < whole)
        def _():
            block(j, False)

        @pl.when(j == whole)
        def _():
            block(j, True)

    lax.fori_loop(0, blocks // per, step, None)
    done, end = _steps(blocks, per), BWD_WHEN[-1] + BWD_EVERY * (BWD_ROUNDS - 1) + 1
    if end > done:

        @pl.when(i == blocks - 1)
        def _():
            lax.fori_loop(done, end, lambda t, _: hook(t), None)

    rows = pl.ds(pl.multiple_of(i * bq, bq), bq)
    cos, sin = cos_ref[rows, :], sin_ref[rows, :]
    for h in range(HEADS):
        n, k = h // BWD_STRIP, h % BWD_STRIP
        dq_ref[:, _head(h)] = _turn((dq_s[n, :, k * bq : (k + 1) * bq] * scale).T, cos, -sin).astype(BF16)

    @pl.when(i == pl.num_programs(0) - 1)
    def _():
        def turn(n, _):
            here = pl.ds(pl.multiple_of(n * 256, 256), 256)
            for h in range(KV):
                dk_ref[here, _head(h)] = _turn(dk_s[h, here, :] * scale, cos_ref[here, :], -sin_ref[here, :]).astype(BF16)
                dv_ref[here, _head(h)] = dv_s[h, here, :].astype(BF16)

        lax.fori_loop(0, dk_ref.shape[0] // 256, turn, None)
        for j in jobs:
            j.end()


def attend_bwd(q, k, v, o, do, lse, cos, sin, gg, gu, gd):
    tokens = q.shape[0]
    anywhere = pl.BlockSpec(memory_space=pl.ANY)
    block = pl.BlockSpec((BWD_Q, HEADS * HEAD), lambda i: (i, 0))
    fixed = lambda a: pl.BlockSpec(a.shape, lambda i: (0, 0))
    wide = BWD_STRIP * BWD_Q
    grads = [g.reshape(SIDE, SIDE, SIDE, g.shape[0] // 64, g.shape[1]) for g in (gg, gu, gd)]
    return pl.pallas_call(
        _attend_bwd,
        grid=(tokens // BWD_Q,),
        out_shape=[jax.ShapeDtypeStruct(q.shape, BF16), jax.ShapeDtypeStruct(k.shape, BF16), jax.ShapeDtypeStruct(v.shape, BF16)]
        + [jax.ShapeDtypeStruct(g.shape[3:], BF16) for g in grads],
        in_specs=[block, fixed(k), fixed(v), block, block, pl.BlockSpec((HEADS, BWD_Q), lambda i: (0, i)), fixed(cos), fixed(sin)]
        + [anywhere] * 3,
        out_specs=[block, fixed(k), fixed(v)] + [anywhere] * 3,
        scratch_shapes=[pltpu.VMEM((HEADS // BWD_STRIP, HEAD, wide), F32), pltpu.VMEM((KV, tokens, HEAD), F32),
                        pltpu.VMEM((KV, tokens, HEAD), F32), pltpu.VMEM((BWD_K, wide), jnp.int32)]
        + [s for g in grads for s in Scatter.scratch(g.shape[3], g.shape[4] // BWD_ROUNDS, BWD_ROUNDS)],
        compiler_params=pltpu.CompilerParams(collective_id=2, has_side_effects=True, vmem_limit_bytes=60 * 2**20,
                                             dimension_semantics=("arbitrary",)),
        name="attend_bwd",
    )(q, k, v, o, do, lse, cos, sin, *grads)


def _last(gq, gk, gv, go, oq, ok, ov, oo, *scratch):
    place = Place()
    each = len(scratch) // 6
    plan = last_plan(gq, go)
    pairs = dict(q=(gq, oq), k=(gk, ok), v=(gv, ov), o=(go, oo))
    jobs = [Scatter(place, *pairs[name], colour, at, width, 1, scratch[n * each : (n + 1) * each])
            for n, (name, colour, at, width) in enumerate(plan)]
    meet(place, False, False)
    for s in range(SCATTER_STAGES):
        for j in jobs:
            j.stage(s, 0)
    for j in jobs:
        j.end()


def last_plan(gq, go):
    return (("q", 0, 0, 1024), ("o", 1, 0, 768), ("q", 2, 1024, 512), ("o", 2, 768, 256), ("k", 2, 0, 256), ("v", 2, 0, 256))


def last(gq, gk, gv, go):
    anywhere = pl.BlockSpec(memory_space=pl.ANY)
    grads = dict(zip("qkvo", [g.reshape(SIDE, SIDE, SIDE, g.shape[0] // 64, g.shape[1]) for g in (gq, gk, gv, go)]))
    return pl.pallas_call(
        _last,
        out_shape=[jax.ShapeDtypeStruct(g.shape[3:], BF16) for g in grads.values()],
        in_specs=[anywhere] * 4,
        out_specs=[anywhere] * 4,
        scratch_shapes=[s for name, _, _, width in last_plan(gq, go) for s in Scatter.scratch(grads[name].shape[3], width, 1)],
        compiler_params=pltpu.CompilerParams(collective_id=3, has_side_effects=True, vmem_limit_bytes=48 * 2**20),
        name="last",
    )(*grads.values())


def matmul(a, w, ca=1, cb=0):
    return _dot(a, w, ca, cb).astype(BF16)


def scale_of(h):
    wide = h.astype(F32)
    return lax.rsqrt(jnp.mean(wide * wide, -1, keepdims=True) + EPS)


def norm_bwd(h, scale, by):
    h, by = h.astype(F32), by.astype(F32)
    return scale * (by - h * (scale * scale * jnp.mean(h * by, -1, keepdims=True)))


def tables(tokens):
    half = HEAD // 2
    angle = jnp.arange(tokens, dtype=F32)[:, None] * THETA ** (-jnp.arange(half, dtype=F32) / half)
    cos, sin = jnp.cos(angle), jnp.sin(angle)
    return jnp.concatenate([cos, cos], 1), jnp.concatenate([-sin, sin], 1)


def layer(x, dy, wq, wk, wv, wo, wg, wu, wd):
    cos, sin = tables(x.shape[0])
    a, (wq, wk, wv) = first(x, wq, wk, wv)
    (o, lse, q, k), (wo, wg, wu, wd) = attend(matmul(a, wq), matmul(a, wk), v := matmul(a, wv), cos, sin, wo, wg, wu, wd)
    h = x + matmul(o, wo)
    scale = scale_of(h)
    b = (h.astype(F32) * scale).astype(BF16)
    gate, up = _dot(b, wg, 1, 0), _dot(b, wu, 1, 0)
    act = (jax.nn.silu(gate) * up).astype(BF16)
    d_act = matmul(dy, wd, 1, 1).astype(F32)
    g_down = matmul(act, dy, 0, 0)
    sig = jax.nn.sigmoid(gate)
    d_gate = (d_act * up * sig * (1 + gate * (1 - sig))).astype(BF16)
    d_up = (d_act * gate * sig).astype(BF16)
    g_gate, g_up = matmul(b, d_gate, 0, 0), matmul(b, d_up, 0, 0)
    d_b = _dot(d_gate, wg, 1, 1) + _dot(d_up, wu, 1, 1)
    d_h = (dy.astype(F32) + norm_bwd(h, scale, d_b)).astype(BF16)
    g_o = matmul(o, d_h, 0, 0)
    dq, dk, dv, g_gate, g_up, g_down = attend_bwd(q, k, v, o, matmul(d_h, wo, 1, 1), lse, cos, sin, g_gate, g_up, g_down)
    g_q, g_k, g_v = matmul(a, dq, 0, 0), matmul(a, dk, 0, 0), matmul(a, dv, 0, 0)
    g_q, g_k, g_v, g_o = last(g_q, g_k, g_v, g_o)
    d_a = _dot(dq, wq, 1, 1) + _dot(dk, wk, 1, 1) + _dot(dv, wv, 1, 1)
    d_x = (d_h.astype(F32) + norm_bwd(x, scale_of(x), d_a)).astype(BF16)
    return d_x, g_q, g_k, g_v, g_o, g_gate, g_up, g_down


def solution(mesh):
    def step(x, dy, *weights):
        return tuple(out[None] for out in layer(x[0], dy[0], *(w[0] for w in weights)))

    states, cut = P(("rep", "dp"), None, None), P(None, "dp", None)
    return jax.shard_map(
        step,
        mesh=mesh,
        in_specs=(states, states) + (cut,) * 7,
        out_specs=(states,) + (P("rep", "dp", None),) * 7,
        check_vma=False,
    )
```

```python
import functools
import math

import jax
import jax.numpy as jnp
from jax import lax
from jax.experimental import pallas as pl
from jax.experimental.pallas import tpu as pltpu
from jax.sharding import PartitionSpec as P

MESH = pl.DeviceIdType.MESH
BF16, F32 = jnp.bfloat16, jnp.float32
HEAD = 128
HEADS = 12
KV = 2
GROUP = HEADS // KV
THETA = 10000
EPS = 1e-6
LOG2E = 1.4426950408889634
HIDDEN = -2e30
SIDE = 4
ORDERS = ((0, 1, 2), (1, 2, 0), (2, 0, 1))


def _dot(a, b, ca, cb):
    return lax.dot_general(a, b, (((ca,), (cb,)), ((), ())), preferred_element_type=F32)


class Place:
    def __init__(self):
        self.rep, p = lax.axis_index("rep"), lax.axis_index("dp")
        self.at = (p // 16, (p // 4) % 4, p % 4)

    def step(self, dim, by):
        return (self.at[dim] + by) % SIDE

    def device(self, dim, by):
        x, y, z = (self.step(d, by) if d == dim else self.at[d] for d in range(3))
        return (self.rep, x * 16 + y * 4 + z)

    def partner(self):
        x, y, z = self.at
        return (1 - self.rep, x * 16 + y * 4 + z)


def meet(place, far, partner):
    others = [place.device(d, by) for d in range(3) for by in ((1, 3, 2) if far else (1, 3))]
    if partner:
        others.append(place.partner())
    barrier = pltpu.get_barrier_semaphore()
    for other in others:
        pl.semaphore_signal(barrier, inc=1, device_id=other, device_id_type=MESH)
    pl.semaphore_wait(barrier, len(others))


COPIES = 15
GATHER_STAGES = 7


class Gather:
    def __init__(self, place, shard, full, colour, first, width, send, recv, local):
        self.place, self.shard, self.full, self.dims = place, shard, full, ORDERS[colour]
        half = shard.shape[-1] // 2
        self.cols = pl.ds(pl.multiple_of(place.rep * half + first, 128), width)
        self.send, self.recv, self.local = send, recv, local

    def blocks(self, **where):
        index = [slice(None)] * 3
        for name, value in where.items():
            index[self.dims[int(name[1])]] = value
        return self.full.at[(*index, slice(None), self.cols)]

    def copies(self):
        p, (a, b, c) = self.place, self.dims
        ia, ib, ic = (p.at[d] for d in self.dims)
        low, high = pl.ds(0, 2), pl.ds(2, 2)
        own = self.blocks(d0=ia, d1=ib, d2=ic)
        mine = self.shard.at[:, self.cols]
        out = [(mine, own, p.device(a, by)) for by in (1, 3, 2)]
        row = self.blocks(d1=ib, d2=ic)
        out += [(row, row, p.device(b, by)) for by in (1, 3)]
        for by, part in ((1, low), (3, high)):
            got = self.blocks(d0=part, d1=p.step(b, -by), d2=ic)
            out.append((got, got, p.device(b, by)))
        plane = self.blocks(d2=ic)
        out += [(plane, plane, p.device(c, by)) for by in (1, 3)]
        for by, part in ((1, low), (3, high)):
            got = self.blocks(d0=part, d2=p.step(c, -by))
            out.append((got, got, p.device(c, by)))
        for by in (0, 1, 3, 2):
            got = self.blocks(d2=p.step(c, by))
            out.append((got, got, p.partner()))
        return out

    def copy(self, n):
        src, dst, device = self.copies()[n]
        return pltpu.make_async_remote_copy(src_ref=src, dst_ref=dst, send_sem=self.send.at[n], recv_sem=self.recv.at[n], device_id=device,
                                            device_id_type=MESH)

    def keep(self):
        ia, ib, ic = (self.place.at[d] for d in self.dims)
        return pltpu.make_async_copy(self.shard.at[:, self.cols], self.blocks(d0=ia, d1=ib, d2=ic), self.local)

    def start(self, *which):
        for n in which:
            self.copy(n).start()

    def got(self, *which):
        for n in which:
            self.copy(n).wait_recv()

    def stage(self, s):
        if s == 0:
            self.keep().start()
            self.start(0, 1, 2)
        elif s == 1:
            self.keep().wait()
            self.got(0, 1, 2)
            self.start(3, 4)
        elif s == 2:
            self.got(3, 4)
            self.start(5, 6)
        elif s == 3:
            self.got(5, 6)
            self.start(7, 8, 11)
        elif s == 4:
            self.got(7, 8)
            self.start(9, 10, 12, 13)
        elif s == 5:
            self.got(9, 10)
            self.start(14)
        else:
            self.got(11, 12, 13, 14)
            for n in range(COPIES):
                self.copy(n).wait_send()


SCATTER_STAGES = 7
SLOTS = 3


class Scatter:
    def __init__(self, place, source, target, colour, rounds, rows, width, scratch, here=False):
        self.place, self.source, self.target, self.rounds, self.rows, self.width, self.here = place, source, target, rounds, rows, width, here
        self.dims = ORDERS[colour]
        self.left = [[d for d in range(3) if d not in self.dims[: n + 1]] for n in range(3)]
        scratch = list(scratch)
        (self.ra0, self.rb0, self.x1, self.ra1, self.rb1, self.x2, self.ra2, self.rb2, self.total, self.send0, self.recv0, self.send1, self.recv1,
         self.save) = scratch[:14]
        if not here:
            self.own, self.rel, self.load = scratch[14:]

    @staticmethod
    def scratch(rows, width, rounds, here=False):
        slots = min(SLOTS, rounds)
        b0, b1, b2 = (4, 4, rows, width), (4, rows, width), (rows, width)
        h0, h1, h2 = (2, 4, rows, width), (2, rows, width), (rows // 2, width) if width % 256 else (rows, width // 2)
        vmem = lambda *shape: pltpu.VMEM(shape, BF16)
        dma = pltpu.SemaphoreType.DMA
        out = [vmem(slots, 2, *h0), vmem(slots, 2, *b0), vmem(rounds, *b0), vmem(rounds, 2, *h1), vmem(rounds, 2, *b1), vmem(rounds, *b1),
               vmem(rounds, 2, *h2), vmem(rounds, 2, *b2), vmem(rounds, *b2), dma((slots, 6)), dma((slots, 6)), dma((rounds, 2, 6)),
               dma((rounds, 2, 6)), dma((rounds,))]
        return out if here else out + [vmem(slots, *b0), vmem(slots, 2, *h0), dma((slots, 3))]

    def slot(self, r):
        return r % min(SLOTS, self.rounds)

    def part(self, n, half):
        if n < 2:
            return (pl.ds(2 * half, 2),)
        if self.width % 256:
            return (pl.ds(half * (self.rows // 2), self.rows // 2), slice(None))
        return (slice(None), pl.ds(half * (self.width // 2), self.width // 2))

    def x(self, n, r, j, half=None):
        d = self.dims[n]
        rest = () if half is None else self.part(n, half)
        if n == 0:
            index = [slice(None)] * 3
            index[d] = j
            if half is not None:
                index[self.left[0][0]] = rest[0]
            return self.source(r, tuple(index))
        if n == 1:
            index = [slice(None)] * 2
            index[self.left[0].index(d)] = j
            if half is not None:
                index[self.left[0].index(self.left[1][0])] = rest[0]
            return self.x1.at[(r, *index)]
        return self.x2.at[(r, j, *rest)]

    def copy(self, n, r, k):
        p, d = self.place, self.dims[n]
        by, half = (1, 3)[k % 2], (0, 1, 1, 0, 0, 1)[k]
        s = self.slot(r)
        ra, rb = ((self.ra0.at[s], self.rb0.at[s]), (self.ra1.at[r], self.rb1.at[r]), (self.ra2.at[r], self.rb2.at[r]))[n]
        send, recv = (self.send0.at[s], self.recv0.at[s]) if n == 0 else (self.send1.at[r, n - 1], self.recv1.at[r, n - 1])
        if k < 2:
            src, dst = self.x(n, r, p.step(d, 2), half), ra.at[k]
        else:
            dst = rb.at[(k % 2, *self.part(n, half))]
            src = self.rel.at[s, k - 4] if n == 0 and k >= 4 and not self.here else self.x(n, r, p.step(d, by), half)
        return pltpu.make_async_remote_copy(src_ref=src, dst_ref=dst, send_sem=send.at[k], recv_sem=recv.at[k], device_id=p.device(d, by),
                                            device_id_type=MESH)

    def loading(self, r, k):
        p, d, s = self.place, self.dims[0], self.slot(r)
        src = self.x(0, r, p.at[d]) if k == 2 else self.x(0, r, p.step(d, (1, 3)[k]), k)
        return pltpu.make_async_copy(src, self.own.at[s] if k == 2 else self.rel.at[s, k], self.load.at[s, k])

    def saving(self, r):
        return pltpu.make_async_copy(self.total.at[r], self.target(r), self.save.at[r])

    def relay(self, n, r):
        p, d, s = self.place, self.dims[n], self.slot(r)
        for h in range(2):
            ra = (self.ra0.at[s, h], self.ra1.at[r, h], self.ra2.at[r, h])[n]
            mine = self.rel.at[s, h] if n == 0 and not self.here else self.x(n, r, p.step(d, (1, 3)[h]), h)
            _add(mine, [mine, ra])

    def finish(self, n, r):
        p, d, s = self.place, self.dims[n], self.slot(r)
        rb = (self.rb0.at[s], self.rb1.at[r], self.rb2.at[r])[n]
        mine = self.own.at[s] if n == 0 and not self.here else self.x(n, r, p.at[d])
        _add((self.x1.at[r], self.x2.at[r], self.total.at[r])[n], [mine, rb.at[0], rb.at[1]])

    def begin(self, n, r):
        for k in range(4):
            self.copy(n, r, k).start()

    def stage(self, s, r):
        if s == 0:
            self.begin(0, r)
            if not self.here:
                for k in range(3):
                    self.loading(r, k).start()
            return
        n = (s - 1) // 2
        load = n == 0 and not self.here
        if s % 2:
            for k in (0, 1):
                self.copy(n, r, k).wait_recv()
                if load:
                    self.loading(r, k).wait()
            self.relay(n, r)
            for k in (4, 5):
                self.copy(n, r, k).start()
            return
        for k in (2, 3, 4, 5):
            self.copy(n, r, k).wait_recv()
        if load:
            self.loading(r, 2).wait()
        self.finish(n, r)
        if n < 2:
            self.begin(n + 1, r)
        else:
            self.saving(r).start()
        for k in range(6):
            self.copy(n, r, k).wait_send()

    def end(self):
        for r in range(self.rounds):
            self.saving(r).wait()


def blocks_of(ref, first, width):
    return lambda r, index: ref.at[(*index, slice(None), pl.ds(pl.multiple_of(first + r * width, 128), width))]


def rounds_of(ref, first=0):
    return lambda r, index: ref.at[(first + r, *index)]


def columns_of(ref, first, width):
    return lambda r: ref.at[:, pl.ds(pl.multiple_of(first + r * width, 128), width)]


def run(jobs, when, every, t):
    for s in reversed(range(SCATTER_STAGES)):
        since = t - when[s]

        @pl.when((since >= 0) & (since < every * max(j.rounds for j in jobs)) & (since % every == 0))
        def _(s=s, since=since):
            r = since // every
            for rounds in sorted({j.rounds for j in jobs}):

                @pl.when(r < rounds)
                def _():
                    for j in jobs:
                        if j.rounds == rounds:
                            j.stage(s, r)


def last_due(jobs, when, every):
    return when[-1] + every * (max(j.rounds for j in jobs) - 1)


def _add(out, terms):
    lead = out.shape[:-2]
    if not lead:
        out[...] = sum(t[...].astype(F32) for t in terms).astype(out.dtype)
        return

    def one(i, _):
        index = []
        for size in reversed(lead):
            index.insert(0, i % size)
            i = i // size
        index = tuple(index)
        out[index] = sum(t[index].astype(F32) for t in terms).astype(out.dtype)

    lax.fori_loop(0, math.prod(lead), one, None)


def _first(x_ref, q_in, k_in, v_in, a_ref, q_out, k_out, v_out, send, recv, local):
    place = Place()
    job = lambda n, shard, full, colour, first, width: Gather(place, shard, full, colour, first, width, send.at[n], recv.at[n], local.at[n])
    wide = q_in.shape[1] // 4
    jobs = [job(0, q_in, q_out, 0, 0, wide), job(1, q_in, q_out, 1, wide, wide), job(2, k_in, k_out, 2, 0, k_in.shape[1] // 2),
            job(3, v_in, v_out, 2, 0, v_in.shape[1] // 2)]
    meet(place, True, True)
    for j in jobs:
        j.stage(0)

    rows = 128

    def norm(i, _):
        here = pl.ds(pl.multiple_of(i * rows, rows), rows)
        wide = x_ref[here, :].astype(F32)
        a_ref[here, :] = (wide * lax.rsqrt(jnp.mean(wide * wide, -1, keepdims=True) + EPS)).astype(BF16)

    lax.fori_loop(0, x_ref.shape[0] // rows, norm, None)
    for s in range(1, GATHER_STAGES):
        for j in jobs:
            j.stage(s)


def torus(w):
    return (SIDE, SIDE, SIDE, w.shape[0], w.shape[1])


def first(x, wq, wk, wv):
    anywhere = pl.BlockSpec(memory_space=pl.ANY)
    vmem = pl.BlockSpec(memory_space=pltpu.VMEM)
    dma = pltpu.SemaphoreType.DMA
    full = lambda w: jax.ShapeDtypeStruct(torus(w), BF16)
    out = pl.pallas_call(
        _first,
        out_shape=[jax.ShapeDtypeStruct(x.shape, BF16), full(wq), full(wk), full(wv)],
        in_specs=[vmem, anywhere, anywhere, anywhere],
        out_specs=[vmem, anywhere, anywhere, anywhere],
        scratch_shapes=[dma((4, COPIES)), dma((4, COPIES)), dma((4,))],
        compiler_params=pltpu.CompilerParams(collective_id=0, has_side_effects=True, vmem_limit_bytes=32 * 2**20),
        name="first",
    )(x, wq, wk, wv)
    return out[0], [w.reshape(-1, w.shape[-1]) for w in out[1:]]


def _steps(i, per):
    m, k = i // per, i % per
    return per * (m * (m + 1) // 2) + k * (m + 1)


def _turn(x, cos, sin):
    return x * cos + pltpu.roll(x, HEAD // 2, 1) * sin


def _head(h):
    return slice(h * HEAD, (h + 1) * HEAD)


FWD_Q, FWD_K, FWD_STRIP = 256, 512, 2
BWD_Q, BWD_K, BWD_STRIP = 128, 512, 3
FWD_WHEN = (0, 2, 4, 7, 10, 14, 18)


def _attend(q_ref, k_ref, v_ref, cos_ref, sin_ref, o_in, g_in, u_in, d_in, out_ref, lse_ref, qr_ref, kr_ref, o_out, g_out, u_out, d_out,
            q_s, top_s, mix_s, gap_s, send, recv, local):
    i = pl.program_id(0)
    bq, bk, per = q_ref.shape[0], FWD_K, FWD_K // FWD_Q
    wide = FWD_STRIP * bq
    e = HEAD**-0.5 * LOG2E
    strips = HEADS // FWD_STRIP
    place = Place()
    job = lambda n, shard, full, colour, first, width: Gather(place, shard, full, colour, first, width, send.at[n], recv.at[n], local.at[n])
    jobs = [job(0, o_in, o_out, 0, 0, 128), job(1, o_in, o_out, 1, 128, 128), job(2, o_in, o_out, 2, 256, 256),
            job(3, g_in, g_out, 0, 0, g_in.shape[1] // 2), job(4, u_in, u_out, 1, 0, u_in.shape[1] // 2),
            job(5, d_in, d_out, 2, 0, d_in.shape[1] // 2)]

    @pl.when(i == 0)
    def _():
        meet(place, True, True)

    def hook(t):
        for s, due in enumerate(FWD_WHEN):

            @pl.when(t == due)
            def _(s=s):
                for j in jobs:
                    j.stage(s)

    @pl.when(i == 0)
    def _():
        gap_s[...] = lax.broadcasted_iota(jnp.int32, gap_s.shape, 1) % bq - lax.broadcasted_iota(jnp.int32, gap_s.shape, 0)

        def turn(n, _):
            here = pl.ds(pl.multiple_of(n * 256, 256), 256)
            for h in range(KV):
                kr_ref[here, _head(h)] = _turn(k_ref[here, _head(h)].astype(F32), cos_ref[here, :], sin_ref[here, :]).astype(BF16)

        lax.fori_loop(0, k_ref.shape[0] // 256, turn, None)

    rows = pl.ds(pl.multiple_of(i * bq, bq), bq)
    cos, sin = cos_ref[rows, :], sin_ref[rows, :]
    for h in range(HEADS):
        turned = _turn(q_ref[:, _head(h)].astype(F32), cos, sin).astype(BF16)
        qr_ref[:, _head(h)] = turned
        q_s[h // FWD_STRIP, (h % FWD_STRIP) * bq : (h % FWD_STRIP + 1) * bq, :] = turned
    top_s[...] = jnp.full(top_s.shape, HIDDEN / 2, F32)
    mix_s[...] = jnp.zeros(mix_s.shape, F32)
    ones = jnp.ones((8, bk), BF16)

    def block(j, masked):
        here = pl.ds(pl.multiple_of(j * bk, bk), bk)
        kv = lambda n: _head(n * FWD_STRIP // GROUP)
        scores = [_dot(kr_ref[here, kv(n)], q_s[n], 1, 1) for n in range(strips)]
        ok = gap_s[...] >= j * bk - i * bq if masked else None
        weights, keeps = [], []
        for n, s in enumerate(scores):
            if masked:
                s = jnp.where(ok, s, HIDDEN)
            old = top_s[n : n + 1, :]
            top = jnp.maximum(old, s.max(axis=0, keepdims=True))
            top_s[n : n + 1, :] = top
            weights.append(jnp.exp2((s - top) * e).astype(BF16))
            keeps.append(jnp.exp2((old - top) * e))
        for n, (p, keep) in enumerate(zip(weights, keeps)):
            values = jnp.concatenate([v_ref[here, kv(n)].T, ones], axis=0)
            mix_s[n] = mix_s[n] * keep + _dot(values, p, 1, 0)

    whole, base = i // per, _steps(i, per)
    blocks = q_tokens(cos_ref) // bq

    def step(j, _):
        @pl.when(j <= whole)
        def _():
            hook(base + j)

        @pl.when(j < whole)
        def _():
            block(j, False)

        @pl.when(j == whole)
        def _():
            block(j, True)

    lax.fori_loop(0, blocks // per, step, None)
    done = _steps(blocks, per)
    if FWD_WHEN[-1] >= done:

        @pl.when(i == blocks - 1)
        def _():
            lax.fori_loop(done, FWD_WHEN[-1] + 1, lambda t, _: hook(t), None)

    for h in range(HEADS):
        n, at = h // FWD_STRIP, slice((h % FWD_STRIP) * bq, (h % FWD_STRIP + 1) * bq)
        total = mix_s[n, HEAD : HEAD + 1, at]
        out_ref[:, _head(h)] = (mix_s[n, :HEAD, at] * (1 / total)).T.astype(BF16)
        lse_ref[h : h + 1, :] = (top_s[n : n + 1, at] * HEAD**-0.5 + jnp.log(total)) * LOG2E


def q_tokens(ref):
    return ref.shape[0]


def attend(q, k, v, cos, sin, wo, wg, wu, wd):
    tokens = q.shape[0]
    anywhere = pl.BlockSpec(memory_space=pl.ANY)
    dma = pltpu.SemaphoreType.DMA
    block = pl.BlockSpec((FWD_Q, HEADS * HEAD), lambda i: (i, 0))
    fixed = lambda a: pl.BlockSpec(a.shape, lambda i: (0, 0))
    full = lambda w: jax.ShapeDtypeStruct(torus(w), BF16)
    wide = FWD_STRIP * FWD_Q
    out = pl.pallas_call(
        _attend,
        grid=(tokens // FWD_Q,),
        out_shape=[jax.ShapeDtypeStruct(q.shape, BF16), jax.ShapeDtypeStruct((HEADS, tokens), F32), jax.ShapeDtypeStruct(q.shape, BF16),
                   jax.ShapeDtypeStruct(k.shape, BF16), full(wo), full(wg), full(wu), full(wd)],
        in_specs=[block, fixed(k), fixed(v), fixed(cos), fixed(sin)] + [anywhere] * 4,
        out_specs=[block, pl.BlockSpec((HEADS, FWD_Q), lambda i: (0, i)), block, fixed(k)] + [anywhere] * 4,
        scratch_shapes=[pltpu.VMEM((HEADS // FWD_STRIP, wide, HEAD), BF16), pltpu.VMEM((HEADS // FWD_STRIP, wide), F32),
                        pltpu.VMEM((HEADS // FWD_STRIP, HEAD + 8, wide), F32), pltpu.VMEM((FWD_K, wide), jnp.int32),
                        dma((6, COPIES)), dma((6, COPIES)), dma((6,))],
        compiler_params=pltpu.CompilerParams(collective_id=1, has_side_effects=True, vmem_limit_bytes=56 * 2**20,
                                             dimension_semantics=("arbitrary",)),
        name="attend",
    )(q, k, v, cos, sin, wo, wg, wu, wd)
    return out[:4], [w.reshape(-1, w.shape[-1]) for w in out[4:]]


TILE = 256
CHUNK = 512
MLP_HOOKS = 7
MLP_WHEN = (4, 8, 12, 15, 18, 21, 24)
MLP_LEFT = 3


def _mlp(b_ref, bt_ref, dy_ref, dyt_ref, wg_ref, wu_ref, wd_ref, db_ref, gd_ref, gg_ref, gu_ref, og, ou, act_s, dg_s, du_s, xg, xu, *scratch):
    i = pl.program_id(0)
    tokens, tiles = b_ref.shape[0], og.shape[1] // TILE + MLP_LEFT
    rows = b_ref.shape[1] // 64
    place = Place()
    each = len(scratch) // 2
    jobs = [Scatter(place, lambda r, index, x=x: x.at[(r % 2, *index)], columns_of(o, 0, TILE), colour, tiles - MLP_LEFT, rows, TILE,
                    scratch[n * each : (n + 1) * each], here=True) for n, (x, o, colour) in enumerate(((xg, og, 0), (xu, ou, 2)))]

    @pl.when(i == 0)
    def _():
        meet(place, False, False)
        db_ref[...] = jnp.zeros(db_ref.shape, F32)

    def forward(m):
        here = slice(m, m + CHUNK)
        b, dy = b_ref[here, :], dy_ref[here, :]
        gate, up, by = _dot(b, wg_ref[...], 1, 0), _dot(b, wu_ref[...], 1, 0), _dot(dy, wd_ref[...], 1, 1).astype(BF16).astype(F32)
        sig = 1 / (1 + jnp.exp2(gate * -LOG2E))
        silu = gate * sig
        act_s[here, :] = (silu * up).astype(BF16)
        dg_s[here, :] = (by * up * (sig + silu * (1 - sig))).astype(BF16)
        du_s[here, :] = (by * silu).astype(BF16)

    def backward(m):
        here = slice(m, m + CHUNK)
        db_ref[here, :] += _dot(dg_s[here, :], wg_ref[...], 1, 1) + _dot(du_s[here, :], wu_ref[...], 1, 1)

    def weight(by_s, x, left):
        grad = _dot(bt_ref[...], by_s[...], 1, 0).astype(BF16)
        left[0] = grad
        x[i % 2] = grad.reshape(x.shape[1:])

    chunks = range(0, tokens, CHUNK)
    half = len(chunks) // 2

    def down():
        grad = _dot(dyt_ref[...], act_s[...], 1, 0)
        for n in range(gd_ref.shape[0]):
            gd_ref[n] = grad[n * 128 : (n + 1) * 128, :].T.astype(BF16)

    parts = (lambda: [forward(m) for m in chunks[:half]], lambda: [forward(m) for m in chunks[half:]], lambda: weight(dg_s, xg, gg_ref),
             lambda: weight(du_s, xu, gu_ref), lambda: [backward(m) for m in chunks[:half]], lambda: [backward(m) for m in chunks[half:]], down)

    def segment(n, _):
        run(jobs, MLP_WHEN, MLP_HOOKS, i * MLP_HOOKS + n)
        for k, part in enumerate(parts):

            @pl.when(n == k)
            def _(part=part):
                part()

    lax.fori_loop(0, MLP_HOOKS, segment, None)

    @pl.when(i == tiles - 1)
    def _():
        due = last_due(jobs, MLP_WHEN, MLP_HOOKS)
        if due >= tiles * MLP_HOOKS:
            lax.fori_loop(tiles * MLP_HOOKS, due + 1, lambda t, _: run(jobs, MLP_WHEN, MLP_HOOKS, t), None)
        for j in jobs:
            j.end()


def mlp(b, bt, dy, dyt, wg, wu, wd):
    (tokens, d), ff = b.shape, wg.shape[1]
    tiles, rows = ff // TILE, d // 64
    done = (tiles - MLP_LEFT) * TILE
    vmem = pl.BlockSpec(memory_space=pltpu.VMEM)
    anywhere = pl.BlockSpec(memory_space=pl.ANY)
    x = pltpu.VMEM((2, SIDE, SIDE, SIDE, rows, TILE), BF16)
    tile = pltpu.VMEM((tokens, TILE), BF16)
    across = pl.BlockSpec((d, TILE), lambda i: (0, i))
    left = pl.BlockSpec((1, d, TILE), lambda i: (i // (tiles - MLP_LEFT) * (i - (tiles - MLP_LEFT)), 0, 0))
    return pl.pallas_call(
        _mlp,
        grid=(tiles,),
        out_shape=[jax.ShapeDtypeStruct((tokens, d), F32), jax.ShapeDtypeStruct((d // 128, ff, 128), BF16)]
        + [jax.ShapeDtypeStruct((MLP_LEFT, d, TILE), BF16)] * 2 + [jax.ShapeDtypeStruct((rows, done), BF16)] * 2,
        in_specs=[vmem] * 4 + [across, across, pl.BlockSpec((TILE, d), lambda i: (i, 0))],
        out_specs=[vmem, pl.BlockSpec((d // 128, TILE, 128), lambda i: (0, i, 0)), left, left, anywhere, anywhere],
        scratch_shapes=[tile, tile, tile, x, x] + Scatter.scratch(rows, TILE, tiles - MLP_LEFT, True) * 2,
        compiler_params=pltpu.CompilerParams(collective_id=4, has_side_effects=True, vmem_limit_bytes=60 * 2**20,
                                             dimension_semantics=("arbitrary",)),
        name="mlp",
    )(b, bt, dy, dyt, wg, wu, wd)


BWD_EVERY = 6
BWD_WHEN = (0, 5, 9, 12, 15, 18, 20)


def bwd_jobs(rows, rows_down, rows_o, d):
    return ((0, d // 256, rows_down, 128), (1, d // 256, rows_down, 128), (0, MLP_LEFT, rows, TILE), (2, MLP_LEFT, rows, TILE), (2, 4, rows_o, d // 4))


def _attend_bwd(q_ref, k_ref, v_ref, o_ref, do_ref, lse_ref, cos_ref, sin_ref, gd, gg, gu, go, dq_ref, dk_ref, dv_ref, od, og, ou, oo,
                dq_s, dk_s, dv_s, gap_s, *scratch):
    i = pl.program_id(0)
    bq, bk, per = q_ref.shape[0], BWD_K, BWD_K // BWD_Q
    strips = HEADS // BWD_STRIP
    wide = BWD_STRIP * bq
    scale = HEAD**-0.5
    e = scale * LOG2E
    place = Place()
    plan = bwd_jobs(og.shape[0], od.shape[0], oo.shape[0], od.shape[1])
    each = len(scratch) // len(plan)
    half = plan[0][1]
    refs = ((rounds_of(gd), columns_of(od, 0, 128)), (rounds_of(gd, half), columns_of(od, half * 128, 128)), (rounds_of(gg), columns_of(og, 0, TILE)),
            (rounds_of(gu), columns_of(ou, 0, TILE)), (blocks_of(go, 0, plan[4][3]), columns_of(oo, 0, plan[4][3])))
    jobs = [Scatter(place, *refs[n], *job, scratch[n * each : (n + 1) * each]) for n, job in enumerate(plan)]

    @pl.when(i == 0)
    def _():
        meet(place, False, False)
        gap_s[...] = lax.broadcasted_iota(jnp.int32, gap_s.shape, 1) % bq - lax.broadcasted_iota(jnp.int32, gap_s.shape, 0)
        dk_s[...] = jnp.zeros(dk_s.shape, F32)
        dv_s[...] = jnp.zeros(dv_s.shape, F32)

    hook = lambda t: run(jobs, BWD_WHEN, BWD_EVERY, t)
    dq_s[...] = jnp.zeros(dq_s.shape, F32)
    heads = lambda n: range(n * BWD_STRIP, (n + 1) * BWD_STRIP)
    deltas, lses = [], []
    for n in range(strips):
        products = [do_ref[:, _head(h)].astype(F32) * o_ref[:, _head(h)].astype(F32) for h in heads(n)]
        deltas.append(jnp.concatenate([x.T.sum(axis=0, keepdims=True) for x in products], axis=1))
        lses.append(jnp.concatenate([lse_ref[h : h + 1, :] for h in heads(n)], axis=1))

    def block(j, masked):
        here = pl.ds(pl.multiple_of(j * bk, bk), bk)
        kv = [n * BWD_STRIP // GROUP for n in range(strips)]
        qs = [jnp.concatenate([q_ref[:, _head(h)] for h in heads(n)], axis=0) for n in range(strips)]
        dos = [jnp.concatenate([do_ref[:, _head(h)] for h in heads(n)], axis=0) for n in range(strips)]
        scores = [_dot(k_ref[here, _head(kv[n])], qs[n], 1, 1) for n in range(strips)]
        dps = [_dot(v_ref[here, _head(kv[n])], dos[n], 1, 1) for n in range(strips)]
        ok = gap_s[...] >= j * bk - i * bq if masked else None
        for n in range(strips):
            p = jnp.exp2(scores[n] * e - lses[n])
            if masked:
                p = jnp.where(ok, p, 0.0)
            ds = (p * (dps[n] - deltas[n])).astype(BF16)
            dv_s[kv[n], here, :] += _dot(p.astype(BF16), dos[n], 1, 0)
            dk_s[kv[n], here, :] += _dot(ds, qs[n], 1, 0)
            dq_s[n] += _dot(k_ref[here, _head(kv[n])].T, ds, 1, 0)

    whole, base = i // per, _steps(i, per)
    blocks = q_tokens(cos_ref) // bq

    def step(j, _):
        @pl.when(j <= whole)
        def _():
            hook(base + j)

        @pl.when(j < whole)
        def _():
            block(j, False)

        @pl.when(j == whole)
        def _():
            block(j, True)

    lax.fori_loop(0, blocks // per, step, None)
    done, end = _steps(blocks, per), last_due(jobs, BWD_WHEN, BWD_EVERY) + 1
    if end > done:

        @pl.when(i == blocks - 1)
        def _():
            lax.fori_loop(done, end, lambda t, _: hook(t), None)

    rows = pl.ds(pl.multiple_of(i * bq, bq), bq)
    cos, sin = cos_ref[rows, :], sin_ref[rows, :]
    for h in range(HEADS):
        n, k = h // BWD_STRIP, h % BWD_STRIP
        dq_ref[:, _head(h)] = _turn((dq_s[n, :, k * bq : (k + 1) * bq] * scale).T, cos, -sin).astype(BF16)

    @pl.when(i == pl.num_programs(0) - 1)
    def _():
        def turn(n, _):
            here = pl.ds(pl.multiple_of(n * 256, 256), 256)
            for h in range(KV):
                dk_ref[here, _head(h)] = _turn(dk_s[h, here, :] * scale, cos_ref[here, :], -sin_ref[here, :]).astype(BF16)
                dv_ref[here, _head(h)] = dv_s[h, here, :].astype(BF16)

        lax.fori_loop(0, dk_ref.shape[0] // 256, turn, None)
        for j in jobs:
            j.end()


def attend_bwd(q, k, v, o, do, lse, cos, sin, gd, gg, gu, go):
    tokens = q.shape[0]
    anywhere = pl.BlockSpec(memory_space=pl.ANY)
    block = pl.BlockSpec((BWD_Q, HEADS * HEAD), lambda i: (i, 0))
    fixed = lambda a: pl.BlockSpec(a.shape, lambda i: (0, 0))
    wide = BWD_STRIP * BWD_Q
    gd, gg, gu = (g.reshape(g.shape[0], SIDE, SIDE, SIDE, g.shape[1] // 64, g.shape[2]) for g in (gd, gg, gu))
    go = go.reshape(SIDE, SIDE, SIDE, go.shape[0] // 64, go.shape[1])
    grads = (gd, gg, gu, go)
    mine = [(g.shape[-2], g.shape[0] * g.shape[-1]) for g in grads[:3]] + [go.shape[3:]]
    return pl.pallas_call(
        _attend_bwd,
        grid=(tokens // BWD_Q,),
        out_shape=[jax.ShapeDtypeStruct(q.shape, BF16), jax.ShapeDtypeStruct(k.shape, BF16), jax.ShapeDtypeStruct(v.shape, BF16)]
        + [jax.ShapeDtypeStruct(shape, BF16) for shape in mine],
        in_specs=[block, fixed(k), fixed(v), block, block, pl.BlockSpec((HEADS, BWD_Q), lambda i: (0, i)), fixed(cos), fixed(sin)]
        + [anywhere] * 4,
        out_specs=[block, fixed(k), fixed(v)] + [anywhere] * 4,
        scratch_shapes=[pltpu.VMEM((HEADS // BWD_STRIP, HEAD, wide), F32), pltpu.VMEM((KV, tokens, HEAD), F32),
                        pltpu.VMEM((KV, tokens, HEAD), F32), pltpu.VMEM((BWD_K, wide), jnp.int32)]
        + [s for _, rounds, rows, width in bwd_jobs(mine[1][0], *(m[0] for m in (mine[0], mine[3])), mine[0][1])
           for s in Scatter.scratch(rows, width, rounds)],
        compiler_params=pltpu.CompilerParams(collective_id=2, has_side_effects=True, vmem_limit_bytes=60 * 2**20,
                                             dimension_semantics=("arbitrary",)),
        name="attend_bwd",
    )(q, k, v, o, do, lse, cos, sin, *grads)


LAST_PLAN = (("q", 0, 0, 512), ("q", 1, 512, 512), ("q", 2, 1024, 512), ("k", 0, 0, 256), ("v", 1, 0, 256))


def _last(gq, gk, gv, dq_ref, dk_ref, dv_ref, wq_ref, wk_ref, wv_ref, x_ref, dh_ref, oq, ok, ov, dx_ref, *scratch):
    place = Place()
    each = len(scratch) // len(LAST_PLAN)
    pairs = dict(q=(gq, oq), k=(gk, ok), v=(gv, ov))
    jobs = [Scatter(place, blocks_of(pairs[name][0], at, width), columns_of(pairs[name][1], at, width), colour, 1, oq.shape[0], width,
                    scratch[n * each : (n + 1) * each]) for n, (name, colour, at, width) in enumerate(LAST_PLAN)]
    meet(place, False, False)
    rows = x_ref.shape[0] // 8
    for s in range(8):
        if s < SCATTER_STAGES:
            for j in jobs:
                j.stage(s, 0)
        here = slice(s * rows, (s + 1) * rows)
        by = sum(_dot(d[here, :], w[...], 1, 1) for d, w in ((dq_ref, wq_ref), (dk_ref, wk_ref), (dv_ref, wv_ref)))
        x = x_ref[here, :].astype(F32)
        scale = lax.rsqrt(jnp.mean(x * x, -1, keepdims=True) + EPS)
        by = scale * (by - x * (scale * scale * jnp.mean(x * by, -1, keepdims=True)))
        dx_ref[here, :] = (dh_ref[here, :].astype(F32) + by).astype(BF16)
    for j in jobs:
        j.end()


def last(gq, gk, gv, dq, dk, dv, wq, wk, wv, x, dh):
    anywhere, vmem = pl.BlockSpec(memory_space=pl.ANY), pl.BlockSpec(memory_space=pltpu.VMEM)
    grads = [g.reshape(SIDE, SIDE, SIDE, g.shape[0] // 64, g.shape[1]) for g in (gq, gk, gv)]
    return pl.pallas_call(
        _last,
        out_shape=[jax.ShapeDtypeStruct(g.shape[3:], BF16) for g in grads] + [jax.ShapeDtypeStruct(x.shape, BF16)],
        in_specs=[anywhere] * 3 + [vmem] * 8,
        out_specs=[anywhere] * 3 + [vmem],
        scratch_shapes=[s for _, _, _, width in LAST_PLAN for s in Scatter.scratch(grads[0].shape[3], width, 1)],
        compiler_params=pltpu.CompilerParams(collective_id=3, has_side_effects=True, vmem_limit_bytes=60 * 2**20),
        name="last",
    )(*grads, dq, dk, dv, wq, wk, wv, x, dh)


def matmul(a, w, ca=1, cb=0):
    return _dot(a, w, ca, cb).astype(BF16)


def scale_of(h):
    wide = h.astype(F32)
    return lax.rsqrt(jnp.mean(wide * wide, -1, keepdims=True) + EPS)


def norm_bwd(h, scale, by):
    h, by = h.astype(F32), by.astype(F32)
    return scale * (by - h * (scale * scale * jnp.mean(h * by, -1, keepdims=True)))


def tables(tokens):
    half = HEAD // 2
    angle = jnp.arange(tokens, dtype=F32)[:, None] * THETA ** (-jnp.arange(half, dtype=F32) / half)
    cos, sin = jnp.cos(angle), jnp.sin(angle)
    return jnp.concatenate([cos, cos], 1), jnp.concatenate([-sin, sin], 1)


def layer(x, dy, wq, wk, wv, wo, wg, wu, wd):
    cos, sin = tables(x.shape[0])
    a, (wq, wk, wv) = first(x, wq, wk, wv)
    (o, lse, q, k), (wo, wg, wu, wd) = attend(matmul(a, wq), matmul(a, wk), v := matmul(a, wv), cos, sin, wo, wg, wu, wd)
    h = x + matmul(o, wo)
    scale = scale_of(h)
    b = (h.astype(F32) * scale).astype(BF16)
    d_b, g_down, g_gate, g_up, r_gate, r_up = mlp(b, b.T, dy, dy.T, wg, wu, wd)
    d_h = (dy.astype(F32) + norm_bwd(h, scale, d_b)).astype(BF16)
    g_o = matmul(o, d_h, 0, 0)
    dq, dk, dv, r_down, s_gate, s_up, r_o = attend_bwd(q, k, v, o, matmul(d_h, wo, 1, 1), lse, cos, sin, g_down, g_gate, g_up, g_o)
    g_q, g_k, g_v = matmul(a, dq, 0, 0), matmul(a, dk, 0, 0), matmul(a, dv, 0, 0)
    r_q, r_k, r_v, d_x = last(g_q, g_k, g_v, dq, dk, dv, wq, wk, wv, x, d_h)
    return d_x, r_q, r_k, r_v, r_o, jnp.concatenate([r_gate, s_gate], 1), jnp.concatenate([r_up, s_up], 1), r_down


def solution(mesh):
    def step(x, dy, *weights):
        return tuple(out[None] for out in layer(x[0], dy[0], *(w[0] for w in weights)))

    states, cut = P(("rep", "dp"), None, None), P(None, "dp", None)
    return jax.shard_map(
        step,
        mesh=mesh,
        in_specs=(states, states) + (cut,) * 7,
        out_specs=(states,) + (P("rep", "dp", None),) * 7,
        check_vma=False,
    )
```
